128 devices in a mesh: expert: 8 (over x, core), shard: 16 (over z, y).
Axes of the slice: x: 4, y: 4, z: 4, core: 2. Of those that a mesh axis runs over, the one named last changes fastest.
Arguments:
- tokens: bfloat16 [1024, 4096], P(('expert', 'shard')), may hold values from -6 to 6
- router: bfloat16 [4096, 8], replicated, may hold values from -0.09375 to 0.09375
- expert_ids: int32 [1024, 2], P(('expert', 'shard')), may hold values from 0 to 7, as said below
- w_gate: bfloat16 [8, 4096, 14336], P('expert', None, 'shard'), may hold values from -0.09375 to 0.09375
- w_up: bfloat16 [8, 4096, 14336], P('expert', None, 'shard'), may hold values from -0.09375 to 0.09375
- w_down: bfloat16 [8, 14336, 4096], P('expert', 'shard'), may hold values from -0.046875 to 0.046875
Outputs:
- mixed: bfloat16 [1024, 4096], P(('expert', 'shard'))
The draws below stay inside these ranges and needn't reach their ends.
Inputs may be any that keep to these rules, and one draw needn't show every extreme that they name: `expert_ids`: each row names 2 different experts. Within the rows of one device no expert is named more than 4 times, and on every device some expert is named exactly 4 times.
All inputs are finite; a program needn't handle non-finite values.
Results may differ from the reference program's by a relative error of at most 0.0074.
Values may be sent and summed in bfloat16 or wider, within the bound.
A program may use at most 128 MiB of HBM per device.

```python
import jax
import jax.numpy as jnp
from jax import lax

D = 4096
FF = 14336
TOP = 2
TOK_DEV = 8
EXPERTS = 8
CAP = 4
TOKENS = 1024


def draw_expert_ids(key, part):
    blocks = TOKENS // TOK_DEV
    base_key = jax.random.fold_in(key, 11)
    key_offset, key_order, key_swap = jax.random.split(base_key, 3)
    block_index = jnp.arange(blocks, dtype=jnp.int32)
    random_offset = jax.random.randint(key_offset, (blocks,), 0, EXPERTS, dtype=jnp.int32)
    offset = jnp.where(block_index % 2 == 1, random_offset, block_index % EXPERTS)
    token_index = jnp.arange(TOK_DEV, dtype=jnp.int32)
    upper = (token_index >= CAP).astype(jnp.int32)
    order_keys = jax.random.split(key_order, blocks)
    orders = jax.vmap(lambda k: jax.random.permutation(k, TOK_DEV))(order_keys).astype(jnp.int32)
    placed = upper[orders]
    first = (offset[:, None] + placed) % EXPERTS
    second = (offset[:, None] + 2 + placed) % EXPERTS
    swapped = jax.random.randint(key_swap, (blocks, TOK_DEV), 0, 2, dtype=jnp.int32)
    lead = jnp.where(swapped == 1, second, first)
    trail = jnp.where(swapped == 1, first, second)
    return jnp.stack([lead, trail], axis=2).reshape(TOKENS, TOP).astype(jnp.int32)


def block_levels(key, extent, shards, smallest, largest):
    factor_of, own = 1.0, jax.random.fold_in(key, 6)
    for dim, blocks in shards:
        heights = jnp.exp(jax.random.uniform(jax.random.fold_in(own, dim), (blocks,), jnp.float32, smallest / len(shards), largest / len(shards)))
        factor_of = factor_of * jnp.repeat(heights, extent[dim] // blocks).reshape([-1 if axis == dim else 1 for axis in range(len(extent))])
    return factor_of


def scatter_about(stream_key, shape, spread, reach, pieces=(), kind=jnp.bfloat16):
    loudness = block_levels(stream_key, shape, pieces, -0.22, 0.18) if pieces else 1.0
    drawn = jax.random.normal(stream_key, shape, jnp.float32) * spread * loudness
    return jnp.minimum(jnp.maximum(drawn, -reach), reach).astype(kind)


def setup_inputs(seed: int = 0) -> dict:
    key_list = jax.random.split(jax.random.key(seed), 7)
    tokens = scatter_about(key_list[0], (TOKENS, D), 1.0, 6.0, ((0, 128),))
    router = scatter_about(key_list[1], (D, EXPERTS), D ** -0.5, 0.09375)
    expert_ids = draw_expert_ids(jax.random.fold_in(key_list[6], 71), 0)
    w_gate = scatter_about(key_list[3], (EXPERTS, D, FF), D ** -0.5, 0.09375, ((0, 8), (2, 16)))
    w_up = scatter_about(key_list[4], (EXPERTS, D, FF), D ** -0.5, 0.09375, ((0, 8), (2, 16)))
    w_down = scatter_about(key_list[5], (EXPERTS, FF, D), FF ** -0.5, 0.046875, ((0, 8), (1, 16)))
    return {"tokens": tokens, "router": router, "expert_ids": expert_ids, "w_gate": w_gate, "w_up": w_up, "w_down": w_down}


def expert_layer(packed):
    rows, gate_w, up_w, down_w = packed
    gate = jnp.dot(rows, gate_w, preferred_element_type=jnp.float32)
    up = jnp.dot(rows, up_w, preferred_element_type=jnp.float32)
    hidden = (jax.nn.silu(gate) * up).astype(jnp.bfloat16)
    return jnp.dot(hidden, down_w, preferred_element_type=jnp.float32).astype(jnp.bfloat16)


def reference(tokens, router, expert_ids, w_gate, w_up, w_down):
    blocks = TOKENS // TOK_DEV
    logits = jnp.dot(tokens, router, preferred_element_type=jnp.float32)
    chosen = jnp.take_along_axis(logits, expert_ids, axis=1)
    first = 1.0 / (1.0 + jnp.exp(-(chosen[:, 0] - chosen[:, 1])))
    gates = jnp.stack([first, 1.0 - first], axis=1)
    grouped = expert_ids.reshape(blocks, TOK_DEV * TOP)
    onehot = (grouped[:, :, None] == jnp.arange(EXPERTS, dtype=jnp.int32)[None, None, :]).astype(jnp.int32)
    before = jnp.cumsum(onehot, axis=1) - onehot
    slots = jnp.sum(before * onehot, axis=2)
    block_ids = jnp.broadcast_to(jnp.arange(blocks, dtype=jnp.int32)[:, None], (blocks, TOK_DEV * TOP))
    positions = (block_ids * CAP + slots).reshape(-1).astype(jnp.int32)
    owners = grouped.reshape(-1).astype(jnp.int32)
    token_index = jnp.repeat(jnp.arange(TOKENS, dtype=jnp.int32), TOP)
    buffer = jnp.zeros((EXPERTS, blocks * CAP, D), jnp.bfloat16)
    buffer = buffer.at[owners, positions].set(tokens[token_index])
    results = lax.map(expert_layer, (buffer, w_gate, w_up, w_down))
    picked = results[owners, positions].reshape(TOKENS, TOP, D).astype(jnp.float32)
    mixed = jnp.sum(gates[:, :, None] * picked, axis=1)
    return mixed.astype(jnp.bfloat16)
```

```python
import jax
import jax.numpy as jnp
from jax import lax
from jax.sharding import PartitionSpec as P


def split_up(x, dim, devices):
    before, after = (x.shape[:dim], x.shape[dim + 1 :])
    return jnp.moveaxis(x.reshape(*before, devices, -1, *after), dim, 0)


def sum_at_owner(x, axis, dim):
    devices = lax.axis_size(axis)
    blocks = lax.all_to_all(split_up(x, dim, devices), axis, 0, 0, tiled=True)
    return jnp.sum(blocks.astype(jnp.float32), axis=0)


def shards(tokens, router, expert_ids, w_gate, w_up, w_down):
    local_tokens = tokens.shape[0]
    width = tokens.shape[1]
    n_experts = router.shape[1]
    slots_per = local_tokens // 2
    logits = jnp.dot(tokens, router, preferred_element_type=jnp.float32)
    lane = jnp.arange(n_experts * slots_per, dtype=jnp.int32)[None, :]
    lane_expert, lane_slot = lane // slots_per, lane % slots_per
    names = [expert_ids[:, k : k + 1] == lane_expert for k in range(expert_ids.shape[1])]
    named = (names[0] | names[1]).astype(jnp.int32)
    before = jnp.cumsum(named, axis=0) - named
    placed = [name & (before == lane_slot) for name in names]
    chosen = [
        jnp.sum(jnp.where(expert_ids[:, k : k + 1] == jnp.arange(n_experts)[None, :], logits, 0.0), axis=1, keepdims=True)
        for k in range(2)
    ]
    first = 1.0 / (1.0 + jnp.exp(-(chosen[0] - chosen[1])))
    gates = [first, 1.0 - first]
    pick = (placed[0] | placed[1]).astype(jnp.bfloat16)
    outgoing = jnp.einsum("ts,td->sd", pick, tokens).astype(jnp.bfloat16)
    outgoing = outgoing.reshape(n_experts, slots_per, width)
    arrived = lax.all_to_all(outgoing, "expert", split_axis=0, concat_axis=0, tiled=True)
    arrived = arrived.reshape(n_experts * slots_per, width)
    rows = lax.all_gather(arrived, "shard", tiled=True)
    gate = jnp.dot(rows, w_gate[0], preferred_element_type=jnp.float32)
    up = jnp.dot(rows, w_up[0], preferred_element_type=jnp.float32)
    hidden = (jax.nn.silu(gate) * up).astype(jnp.bfloat16)
    part = jnp.dot(hidden, w_down[0], preferred_element_type=jnp.float32).astype(jnp.bfloat16)
    summed = sum_at_owner(part, "shard", 0)
    finished = summed.astype(jnp.bfloat16).reshape(n_experts, slots_per, width)
    returned = lax.all_to_all(finished, "expert", split_axis=0, concat_axis=0, tiled=True)
    returned = returned.reshape(n_experts * slots_per, width)
    mix = sum(jnp.where(p, g, 0.0) for p, g in zip(placed, gates))
    mixed = jnp.dot(mix, returned.astype(jnp.float32), precision=lax.Precision.HIGHEST)
    return mixed.astype(jnp.bfloat16)


def solution(mesh):
    placed = (
        P(("expert", "shard"), None),
        P(),
        P(("expert", "shard"), None),
        P("expert", None, "shard"),
        P("expert", None, "shard"),
        P("expert", "shard", None),
    )
    return jax.shard_map(
        shards, mesh=mesh, in_specs=placed, out_specs=P(("expert", "shard"), None), check_vma=False
    )
```

```python
import functools

import jax
import jax.numpy as jnp
from jax import lax
from jax.experimental import pallas as pl
from jax.experimental.pallas import tpu as pltpu
from jax.sharding import PartitionSpec as P

MESH = pl.DeviceIdType.MESH
BF16, F32 = jnp.bfloat16, jnp.float32
ALL = slice(None)

SIDE = 4
HALF = 2048
INFO = 128
GATHER_PARTS = ((0, 768), (768, 768), (1536, 512 + INFO))
SUM_PARTS = ((0, 768), (768, 768), (1536, 512))
ORDERS = ((0, 1, 2), (1, 2, 0), (2, 0, 1))
TILE = 256


def nt_dot(a, b):
    return lax.dot_general(a, b, (((1,), (1,)), ((), ())), preferred_element_type=F32)


def dot(a, b):
    return jnp.dot(a, b, preferred_element_type=F32)


class Place:
    def __init__(self):
        expert, shard = lax.axis_index("expert"), lax.axis_index("shard")
        self.expert = expert
        self.core = expert % 2
        self.own = (expert // 2, shard // SIDE, shard % SIDE)

    def device(self, dim=None, step=0, core=None):
        x, z, y = (
            lax.rem(v + step, SIDE) if d == dim else v for d, v in enumerate(self.own)
        )
        return (x * 2 + (self.core if core is None else core), z * SIDE + y)

    def at(self, dim, step):
        return lax.rem(self.own[dim] + step, SIDE)


def pick(fixed):
    return tuple(fixed.get(d, ALL) for d in range(3))


def routing_info(place, tok, ids, router_t):
    logits = nt_dot(tok, router_t)
    experts = logits.shape[1]
    small = lax.broadcasted_iota(jnp.int32, logits.shape, 1)
    id0, id1 = ids[:, 0:1], ids[:, 1:2]
    chosen = [jnp.sum(jnp.where(small == i, logits, 0.0), axis=1, keepdims=True) for i in (id0, id1)]
    first = 1.0 / (1.0 + jnp.exp(-(chosen[0] - chosen[1])))
    rows = tok.shape[0]
    lane = lax.broadcasted_iota(jnp.int32, (rows, INFO), 1)
    section, of = lane // experts, lane % experts
    is0, is1 = of == id0, of == id1
    gate = jnp.where(is0, first, jnp.where(is1, 1.0 - first, 0.0))
    named = jnp.where(is0 | is1, 1.0, 0.0)
    lower = lax.broadcasted_iota(jnp.int32, (rows, rows), 0) > lax.broadcasted_iota(
        jnp.int32, (rows, rows), 1
    )
    before = dot(jnp.where(lower, 1.0, 0.0).astype(BF16), named.astype(BF16))
    top = gate.astype(BF16).astype(F32)
    middle = (gate - top).astype(BF16).astype(F32)
    low = gate - top - middle
    info = jnp.where(section == 0, top, jnp.where(section == 1, middle, low))
    info = jnp.where(section == 3, named * (before + 1.0), info)
    return jnp.where(section > 3, 0.0, info)


def layer_kernel(
    tok_ref, router_ref, ids_ref, gate_hbm, up_hbm, down_hbm, out_ref,
    wgu, wd, mine, other, rows, scale, place_t, hidden, keep, give, got,
    relay1, final1, relay2, final2, last, w_sems, send_sems, recv_sems,
):
    place = Place()
    experts = router_ref.shape[0]
    ff_tiles = wgu.shape[0]
    width = TILE // 2

    loads = []
    for j in range(ff_tiles):
        span = pl.ds(j * width, width)
        loads.append((gate_hbm.at[0, :, span], wgu.at[j, :, pl.ds(0, width)]))
        loads.append((up_hbm.at[0, :, span], wgu.at[j, :, pl.ds(width, width)]))
    loads.append((down_hbm.at[0], wd))
    loads = [pltpu.make_async_copy(s, d, w_sems.at[i]) for i, (s, d) in enumerate(loads)]
    for copy in loads:
        copy.start()

    barrier = pltpu.get_barrier_semaphore()
    partners = [place.device(d, step) for d in range(3) for step in (1, 2, 3)]
    partners.append(place.device(core=1 - place.core))
    for partner in partners:
        pl.semaphore_signal(barrier, inc=1, device_id=partner, device_id_type=MESH)

    tok = tok_ref[...]
    block = jnp.concatenate([tok[:, :HALF].astype(F32), tok[:, HALF:].astype(F32)], axis=0)
    info = routing_info(place, tok, ids_ref[...], router_ref[...])
    mine[(*place.own, ALL, pl.ds(0, HALF))] = block.astype(BF16)
    mine[(*place.own, ALL, pl.ds(HALF, INFO))] = jnp.concatenate([info, info], axis=0).astype(BF16)
    pl.semaphore_wait(barrier, len(partners))

    started = []

    def send(src, dst, device):
        n = len(started)
        copy = pltpu.make_async_remote_copy(
            src_ref=src, dst_ref=dst, send_sem=send_sems.at[n], recv_sem=recv_sems.at[n],
            device_id=device, device_id_type=MESH,
        )
        copy.start()
        started.append(copy)
        return copy

    def block_slice(ref, part, fixed):
        return ref.at[(*pick(fixed), ALL, pl.ds(*GATHER_PARTS[part]))]

    def spread(part, fixed, dim):
        cut = ORDERS[part][0]
        half = [{**fixed, cut: pl.ds(0, 2)}, {**fixed, cut: pl.ds(2, 2)}]
        sent = {}
        for h, step in ((0, 1), (1, 3), (1, 1), (0, 3)):
            piece = block_slice(mine, part, {**half[h], dim: place.own[dim]})
            sent[h, step] = send(piece, piece, place.device(dim, step))
        return half, sent

    def relay(part, dim, half, sent):
        far = []
        for h, step in ((0, 1), (1, 3)):
            sent[h, step].wait_recv()
            piece = block_slice(mine, part, {**half[h], dim: place.at(dim, 4 - step)})
            far.append(send(piece, piece, place.device(dim, step)))
        return far

    partner = place.device(core=1 - place.core)

    def to_partner(part, fixed):
        return send(block_slice(mine, part, fixed), block_slice(other, part, fixed), partner)

    parts = range(3)
    first = []
    for part in parts:
        d1, d2, d3 = ORDERS[part]
        piece = block_slice(mine, part, dict(enumerate(place.own)))
        first.append([send(piece, piece, place.device(d1, step)) for step in (1, 2, 3)])
    second = []
    for part in parts:
        d1, d2, d3 = ORDERS[part]
        for copy in first[part]:
            copy.wait_recv()
        second.append(spread(part, {d3: place.own[d3]}, d2))
    far2 = [relay(part, ORDERS[part][1], *second[part]) for part in parts]
    third, across = [], []
    for part in parts:
        d1, d2, d3 = ORDERS[part]
        second[part][1][1, 1].wait_recv()
        second[part][1][0, 3].wait_recv()
        for copy in far2[part]:
            copy.wait_recv()
        third.append(spread(part, {}, d3))
        across.append(to_partner(part, {d3: place.own[d3]}))
    far3 = [relay(part, ORDERS[part][2], *third[part]) for part in parts]
    for part in parts:
        d3 = ORDERS[part][2]
        third[part][1][1, 1].wait_recv()
        across.append(to_partner(part, {d3: place.at(d3, 3)}))
        third[part][1][0, 3].wait_recv()
        across.append(to_partner(part, {d3: place.at(d3, 1)}))
    for part in parts:
        d3 = ORDERS[part][2]
        half = third[part][0]
        for h, copy in enumerate(far3[part]):
            copy.wait_recv()
            across.append(to_partner(part, {**half[h], d3: place.at(d3, 2)}))

    r_i = lax.broadcasted_iota(jnp.int32, (128, 256), 0)
    c_i = lax.broadcasted_iota(jnp.int32, (128, 256), 1)
    fits = (c_i // 16 == (r_i % 64) // 4) & ((c_i // 8) % 2 == r_i // 64)
    want = jnp.where(fits, r_i % 4 + 1, -1).astype(F32)
    c_t = lax.broadcasted_iota(jnp.int32, (256, 128), 0)
    r_t = lax.broadcasted_iota(jnp.int32, (256, 128), 1)
    fits_t = (c_t // 16 == (r_t % 64) // 4) & ((c_t // 8) % 2 == r_t // 64)
    want_t = jnp.where(fits_t, r_t % 4 + 1, -1).astype(F32)
    lane8 = lax.broadcasted_iota(jnp.int32, (8, INFO), 1)
    slot_lane = jnp.where(lane8 == 3 * experts + place.expert, 1.0, 0.0).astype(BF16)
    lane_t = lax.broadcasted_iota(jnp.int32, (256, INFO), 1)
    lane64 = lax.broadcasted_iota(jnp.int32, (64, INFO), 1)
    gate_lane = (lane64 % experts == place.expert) & (lane64 < 3 * experts)

    def select(source, base):
        def body(x, carry):
            g = base + x
            info = source[x, :, :, :, pl.ds(HALF, INFO)].reshape(256, INFO)
            code = nt_dot(slot_lane, info)[0:1]
            take = jnp.where(code == want, 1.0, 0.0).astype(BF16)
            code_t = jnp.sum(
                jnp.where(lane_t == 3 * experts + place.expert, info.astype(F32), 0.0),
                axis=1, keepdims=True,
            )
            place_t[g] = jnp.where(code_t == want_t, 1.0, 0.0).astype(BF16)
            gates = jnp.where(gate_lane, dot(take[0:64], info), 0.0)
            scale[g] = jnp.broadcast_to(jnp.sum(gates, axis=1, keepdims=True), (64, width))
            for n in range(0, HALF, 512):
                data = source[x, :, :, :, pl.ds(n, 512)].reshape(256, 512)
                rows[g, :, :, pl.ds(n, 512)] = dot(take, data).astype(BF16).reshape(2, 64, 512)
            return carry

        lax.fori_loop(0, SIDE, body, 0)

    select(mine, 0)
    for copy in across:
        copy.wait_recv()
    select(other, SIDE)

    for copy in loads:
        copy.wait()

    def up_body(j, carry):
        acc = dot(rows[:, 0].reshape(512, HALF), wgu[j, pl.ds(0, HALF), :])
        acc = acc + dot(rows[:, 1].reshape(512, HALF), wgu[j, pl.ds(HALF, HALF), :])
        v, u = acc[:, :width], acc[:, width:]
        act = v / (1.0 + jnp.exp(-v)) * u * scale[...].reshape(512, width)
        hidden[:, pl.ds(pl.multiple_of(j * width, width), width)] = act.astype(BF16)
        return carry

    lax.fori_loop(0, ff_tiles, up_body, 0)

    def project(part):
        start, size = SUM_PARTS[part]
        tiles = size // TILE

        def body(i, carry):
            h, col = i // tiles, pl.multiple_of(start + (i % tiles) * TILE, TILE)
            w = wd[:, pl.ds(pl.multiple_of(h * HALF + col, TILE), TILE)]
            y = dot(hidden[...], w).astype(BF16)
            rows[:, h, :, pl.ds(col, TILE)] = y.reshape(8, 64, TILE)
            return carry

        lax.fori_loop(0, 2 * tiles, body, 0)

    def scatter(part, target, base):
        cols = pl.ds(*SUM_PARTS[part])

        def body(x, carry):
            g = base + x
            y = rows[g, :, :, cols].reshape(128, SUM_PARTS[part][1])
            target[x, :, :, :, cols] = dot(place_t[g], y).astype(BF16).reshape(
                SIDE, SIDE, 16, SUM_PARTS[part][1]
            )
            return carry

        lax.fori_loop(0, SIDE, body, 0)

    def sums(part, fixed):
        return (*pick(fixed), ALL, pl.ds(*SUM_PARTS[part]))

    def add(part, fixed, pieces):
        index = sums(part, fixed)
        total = keep[index].astype(F32)
        for ref, where in pieces:
            total = total + ref[where].astype(F32)
        keep[index] = total.astype(BF16)

    def merge(part):
        def body(x, carry):
            index = (x, ALL, ALL, ALL, pl.ds(*SUM_PARTS[part]))
            keep[index] = (keep[index].astype(F32) + got[index].astype(F32)).astype(BF16)
            return carry

        lax.fori_loop(0, SIDE, body, 0)

    def open_ring(part, dim, cut, fixed, relays, finals):
        half = [{**fixed, cut: pl.ds(0, 2)}, {**fixed, cut: pl.ds(2, 2)}]
        axis = [d for d in range(3) if d not in fixed and d != dim].index(cut)

        def into(ref, way, h):
            index = [ALL] * (len(ref.shape) - 1)
            index[axis] = pl.ds(2 * h, 2)
            return ref.at[(way, *index)]

        sent = {"relay": [], "final": []}
        for h, step in ((0, 1), (1, 3)):
            src = keep.at[sums(part, {**half[h], dim: place.at(dim, 2)})]
            sent["relay"].append(send(src, relays.at[h], place.device(dim, step)))
        for way, h, step in ((0, 1, 1), (1, 0, 3)):
            src = keep.at[sums(part, {**half[h], dim: place.at(dim, step)})]
            sent["final"].append(send(src, into(finals, way, h), place.device(dim, step)))
        return half, into, sent

    def pass_ring(part, dim, relays, finals, half, into, sent):
        for h, step in ((0, 1), (1, 3)):
            sent["relay"][h].wait_recv()
            fixed = {**half[h], dim: place.at(dim, step)}
            add(part, fixed, [(relays, (h,))])
            src = keep.at[sums(part, fixed)]
            sent["final"].append(send(src, into(finals, h, h), place.device(dim, step)))

    def close_ring(part, dim, fixed, finals, sent):
        for copy in sent["final"]:
            copy.wait_recv()
        add(part, {**fixed, dim: place.own[dim]}, [(finals, (0,)), (finals, (1,))])

    rings = {}

    def begin(part):
        across_sum[part].wait_recv()
        merge(part)
        f1, f2, f3 = ORDERS[part]
        rings[part] = open_ring(part, f1, f2, {}, relay1[part], final1[part])

    across_sum = []
    for part in parts:
        project(part)
        scatter(part, give, SIDE)
        cols = pl.ds(*SUM_PARTS[part])
        across_sum.append(
            send(give.at[ALL, ALL, ALL, ALL, cols], got.at[ALL, ALL, ALL, ALL, cols], partner)
        )
        scatter(part, keep, 0)
        if part:
            begin(part - 1)
    begin(2)
    for part in parts:
        pass_ring(part, ORDERS[part][0], relay1[part], final1[part], *rings[part])
    for part in parts:
        f1, f2, f3 = ORDERS[part]
        close_ring(part, f1, {}, final1[part], rings[part][2])
        rings[part] = open_ring(part, f2, f3, {f1: place.own[f1]}, relay2[part], final2[part])
    for part in parts:
        pass_ring(part, ORDERS[part][1], relay2[part], final2[part], *rings[part])
    ends = []
    for part in parts:
        f1, f2, f3 = ORDERS[part]
        close_ring(part, f2, {f1: place.own[f1]}, final2[part], rings[part][2])
        ends.append([])
        for step in (1, 2, 3):
            where = {f1: place.own[f1], f2: place.own[f2], f3: place.at(f3, step)}
            ends[part].append(
                send(keep.at[sums(part, where)], last[part].at[step - 1], place.device(f3, step))
            )
    for part in parts:
        for copy in ends[part]:
            copy.wait_recv()
        start, size = SUM_PARTS[part]
        total = keep[sums(part, dict(enumerate(place.own)))].astype(F32)
        for k in range(3):
            total = total + last[part][k].astype(F32)
        out_ref[:, pl.ds(start, size)] = total[0:8].astype(BF16)
        out_ref[:, pl.ds(HALF + start, size)] = total[8:16].astype(BF16)

    for copy in started:
        copy.wait_send()


def ring_buffers():
    relay1, final1, relay2, final2, last = [], [], [], [], []
    for part, (start, size) in enumerate(SUM_PARTS):
        f1, f2, f3 = ORDERS[part]
        left = [d for d in range(3) if d != f1]
        relay1.append(pltpu.VMEM((2, *(2 if d == f2 else SIDE for d in left), 16, size), BF16))
        final1.append(pltpu.VMEM((2, SIDE, SIDE, 16, size), BF16))
        relay2.append(pltpu.VMEM((2, 2, 16, size), BF16))
        final2.append(pltpu.VMEM((2, SIDE, 16, size), BF16))
        last.append(pltpu.VMEM((3, 16, size), BF16))
    return relay1, final1, relay2, final2, last


COPIES = 108


def layer(tokens, router, expert_ids, w_gate, w_up, w_down):
    depth, ff = w_gate.shape[1], w_gate.shape[2]
    blocks = (SIDE, SIDE, SIDE, 16)
    vmem, anywhere = pl.BlockSpec(memory_space=pltpu.VMEM), pl.BlockSpec(memory_space=pl.ANY)
    return pl.pallas_call(
        layer_kernel,
        out_shape=jax.ShapeDtypeStruct(tokens.shape, BF16),
        in_specs=[vmem, vmem, vmem, anywhere, anywhere, anywhere],
        out_specs=vmem,
        scratch_shapes=[
            pltpu.VMEM((ff // (TILE // 2), depth, TILE), BF16),
            pltpu.VMEM((ff, depth), BF16),
            pltpu.VMEM((*blocks, HALF + INFO), BF16),
            pltpu.VMEM((*blocks, HALF + INFO), BF16),
            pltpu.VMEM((8, 2, 64, HALF), BF16),
            pltpu.VMEM((8, 64, TILE // 2), F32),
            pltpu.VMEM((8, 256, 128), BF16),
            pltpu.VMEM((512, ff), BF16),
            pltpu.VMEM((*blocks, HALF), BF16),
            pltpu.VMEM((*blocks, HALF), BF16),
            pltpu.VMEM((*blocks, HALF), BF16),
            *ring_buffers(),
            pltpu.SemaphoreType.DMA((2 * (ff // (TILE // 2)) + 1,)),
            pltpu.SemaphoreType.DMA((COPIES,)),
            pltpu.SemaphoreType.DMA((COPIES,)),
        ],
        compiler_params=pltpu.CompilerParams(
            collective_id=0, has_side_effects=True, vmem_limit_bytes=67043328
        ),
    )(tokens, router.T, expert_ids, w_gate, w_up, w_down)


def solution(mesh):
    placed = (
        P(("expert", "shard"), None),
        P(),
        P(("expert", "shard"), None),
        P("expert", None, "shard"),
        P("expert", None, "shard"),
        P("expert", "shard", None),
    )
    return jax.shard_map(
        layer, mesh=mesh, in_specs=placed, out_specs=P(("expert", "shard"), None), check_vma=False
    )
```

```python
import functools

import jax
import jax.numpy as jnp
from jax import lax
from jax.experimental import pallas as pl
from jax.experimental.pallas import tpu as pltpu
from jax.sharding import PartitionSpec as P

MESH = pl.DeviceIdType.MESH
BF16, F32 = jnp.bfloat16, jnp.float32
ALL = slice(None)
FIRST, SECOND = ((0, 1), (1, 3)), ((1, 1), (0, 3))

SIDE = 4
HALF = 2048
INFO = 128
DATA = ((0, 0, 768), (768 + INFO, 768, 768), (1536 + INFO, 1536, 512))
ROUTING = 768
GATHER = (
    ((0, 256), (256, 256), (512, 256 + INFO)),
    ((896, 256), (1152, 256), (1408, 256)),
    ((1664, 256), (1920, 256)),
)
ORDERS = ((0, 1, 2), (1, 2, 0), (2, 0, 1))
TILE = 256
CHUNKS = HALF // TILE
DIRECT = 5
GATHER_SEMS, SUM_SEMS = 13, 6


def nt_dot(a, b):
    return lax.dot_general(a, b, (((1,), (1,)), ((), ())), preferred_element_type=F32)


def dot(a, b):
    return jnp.dot(a, b, preferred_element_type=F32)


class Place:
    def __init__(self):
        expert, shard = lax.axis_index("expert"), lax.axis_index("shard")
        self.expert = expert
        self.core = expert % 2
        self.own = (expert // 2, shard // SIDE, shard % SIDE)

    def device(self, dim=None, step=0, core=None):
        x, z, y = (
            lax.rem(v + step, SIDE) if d == dim else v for d, v in enumerate(self.own)
        )
        return (x * 2 + (self.core if core is None else core), z * SIDE + y)

    def at(self, dim, step):
        return lax.rem(self.own[dim] + step, SIDE)


def pick(fixed):
    return tuple(fixed.get(d, ALL) for d in range(3))


def routing_info(place, tok, ids, router_t):
    logits = nt_dot(tok, router_t)
    experts = logits.shape[1]
    small = lax.broadcasted_iota(jnp.int32, logits.shape, 1)
    same = small == lax.broadcasted_iota(jnp.int32, logits.shape, 0)
    id0, id1 = [
        jnp.sum(jnp.where(same, ids[k : k + 1, :], 0), axis=1, keepdims=True) for k in range(2)
    ]
    chosen = [jnp.sum(jnp.where(small == i, logits, 0.0), axis=1, keepdims=True) for i in (id0, id1)]
    first = 1.0 / (1.0 + jnp.exp(-(chosen[0] - chosen[1])))
    rows = tok.shape[0]
    lane = lax.broadcasted_iota(jnp.int32, (rows, INFO), 1)
    section, of = lane // experts, lane % experts
    is0, is1 = of == id0, of == id1
    gate = jnp.where(is0, first, jnp.where(is1, 1.0 - first, 0.0))
    named = jnp.where(is0 | is1, 1.0, 0.0)
    lower = lax.broadcasted_iota(jnp.int32, (rows, rows), 0) > lax.broadcasted_iota(
        jnp.int32, (rows, rows), 1
    )
    before = dot(jnp.where(lower, 1.0, 0.0).astype(BF16), named.astype(BF16))
    top = gate.astype(BF16).astype(F32)
    middle = (gate - top).astype(BF16).astype(F32)
    low = gate - top - middle
    info = jnp.where(section == 0, top, jnp.where(section == 1, middle, low))
    info = jnp.where(section == 3, named * (before + 1.0), info)
    return jnp.where(section > 3, 0.0, info)


def layer_kernel(
    tok_ref, router_ref, ids_ref, gate_hbm, up_hbm, down_hbm, out_ref,
    wgu, wd, mine, other, rows, scale, place_t, sums_gu, hidden, keep, give, got,
    relay1, final1, relay2, final2, last, w_sems, send_sems, recv_sems,
):
    place = Place()
    experts = router_ref.shape[0]
    ff_tiles = wgu.shape[0]
    width = TILE // 2

    loads = []
    for j in range(ff_tiles):
        span = pl.ds(j * width, width)
        loads.append((gate_hbm.at[0, :, span], wgu.at[j, :, pl.ds(0, width)]))
        loads.append((up_hbm.at[0, :, span], wgu.at[j, :, pl.ds(width, width)]))
    loads.append((down_hbm.at[0], wd))
    loads = [pltpu.make_async_copy(s, d, w_sems.at[i]) for i, (s, d) in enumerate(loads)]
    for copy in loads:
        copy.start()

    barrier = pltpu.get_barrier_semaphore()
    partners = [place.device(d, step) for d in range(3) for step in (1, 2, 3)]
    partners.append(place.device(core=1 - place.core))
    for partner in partners:
        pl.semaphore_signal(barrier, inc=1, device_id=partner, device_id_type=MESH)

    tok = tok_ref[...]
    block = jnp.concatenate([tok[:, :HALF].astype(F32), tok[:, HALF:].astype(F32)], axis=0)
    info = routing_info(place, tok, ids_ref[...], router_ref[...])
    block = block.astype(BF16)
    for start, first_col, size in DATA:
        mine[(*place.own, ALL, pl.ds(start, size))] = block[:, first_col : first_col + size]
    mine[(*place.own, ALL, pl.ds(ROUTING, INFO))] = jnp.concatenate([info, info], axis=0).astype(BF16)
    pl.semaphore_wait(barrier, len(partners))

    def send(src, dst, device, kind, arrival):
        pltpu.make_async_remote_copy(
            src_ref=src, dst_ref=dst, send_sem=send_sems.at[kind], recv_sem=recv_sems.at[arrival],
            device_id=device, device_id_type=MESH,
        ).start()

    def waiting(ref, kind, arrival):
        return pltpu.make_async_remote_copy(
            src_ref=ref, dst_ref=ref, send_sem=send_sems.at[kind], recv_sem=recv_sems.at[arrival],
            device_id=partner, device_id_type=MESH,
        )

    def arrive(ref, arrival):
        waiting(ref, 0, arrival).wait_recv()

    partner = place.device(core=1 - place.core)

    def block_slice(ref, chunk, part, fixed):
        return ref.at[(*pick(fixed), ALL, pl.ds(*GATHER[chunk][part]))]

    class Gather:
        def __init__(self, chunk):
            self.chunk, self.parts = chunk, range(len(GATHER[chunk]))
            self.base = chunk * GATHER_SEMS
            start = GATHER[chunk][0][0]
            self.cols = pl.ds(start, sum(size for _, size in GATHER[chunk]))
            for part in self.parts:
                piece = block_slice(mine, chunk, part, dict(enumerate(place.own)))
                for step in (1, 2, 3):
                    send(piece, piece, place.device(ORDERS[part][0], step), 0, self.base)

        def whole(self, fixed):
            return mine.at[(*pick(fixed), ALL, self.cols)]

        def pieces(self, part, fixed, dim, offset, ways, kind, arrival):
            for h, step in ways:
                where = {**fixed, ORDERS[part][0]: pl.ds(2 * h, 2), dim: place.at(dim, offset(step))}
                piece = block_slice(mine, self.chunk, part, where)
                send(piece, piece, place.device(dim, step), kind, arrival)

        def level(self, part, deep):
            d1, d2, d3 = ORDERS[part]
            return ({}, d3, 2) if deep else ({d3: place.own[d3]}, d2, 1)

        def spread(self, part, deep, ways, arrival):
            fixed, dim, kind = self.level(part, deep)
            self.pieces(part, fixed, dim, lambda step: 0, ways, kind, self.base + arrival)

        def relay(self, deep, ready, arrival):
            for part in self.parts:
                fixed, dim, kind = self.level(part, deep)
                size = block_slice(mine, self.chunk, part, {**fixed, dim: place.own[dim]})
                arrive(size, self.base + ready + part)
                self.pieces(
                    part, fixed, dim, lambda step: 4 - step, FIRST, kind, self.base + arrival(part)
                )

        def to_partner(self, step):
            for part in self.parts:
                dim = ORDERS[part][2]
                where = {dim: place.at(dim, step)}
                src = block_slice(mine, self.chunk, part, where)
                dst = block_slice(other, self.chunk, part, where)
                send(src, dst, partner, 3, self.base + 12)

        def spread2(self):
            arrive(self.whole({0: pl.ds(0, 3), 1: 0, 2: 0}), self.base)
            for part in self.parts:
                self.spread(part, False, FIRST, 1 + part)
                self.spread(part, False, SECOND, 4 + part)

        def relay2(self):
            self.relay(False, 1, lambda part: 4 + part)

        def spread3_first(self):
            for part in self.parts:
                d1, d2, d3 = ORDERS[part]
                where = {d2: pl.ds(0, 2), d3: place.own[d3]}
                arrive(block_slice(mine, self.chunk, part, where), self.base + 4 + part)
                self.spread(part, True, FIRST, 7 + part)

        def spread3_second(self):
            for part in self.parts:
                self.spread(part, True, SECOND, 10)
            self.to_partner(0)

        def relay3(self):
            self.relay(True, 7, lambda part: 11)

        def finish(self):
            arrive(self.whole({0: 0}), self.base + 10)
            self.to_partner(1)
            self.to_partner(3)
            arrive(self.whole({0: 0}), self.base + 11)
            self.to_partner(2)

        def wait_across(self):
            arrive(self.whole({}), self.base + 12)

    gathers = [Gather(chunk) for chunk in range(len(GATHER))]
    for g in gathers:
        g.spread2()
    for g in gathers:
        g.relay2()
    gathers[0].spread3_first()
    gathers[0].spread3_second()
    gathers[1].spread3_first()
    gathers[0].relay3()
    gathers[1].spread3_second()
    gathers[2].spread3_first()
    gathers[1].relay3()
    gathers[2].spread3_second()
    gathers[0].finish()

    r_i = lax.broadcasted_iota(jnp.int32, (128, 256), 0)
    c_i = lax.broadcasted_iota(jnp.int32, (128, 256), 1)
    fits = (c_i // 16 == (r_i % 64) // 4) & ((c_i // 8) % 2 == r_i // 64)
    want = jnp.where(fits, r_i % 4 + 1, -1).astype(F32)
    c_t = lax.broadcasted_iota(jnp.int32, (256, 128), 0)
    r_t = lax.broadcasted_iota(jnp.int32, (256, 128), 1)
    fits_t = (c_t // 16 == (r_t % 64) // 4) & ((c_t // 8) % 2 == r_t // 64)
    want_t = jnp.where(fits_t, r_t % 4 + 1, -1).astype(F32)
    lane8 = lax.broadcasted_iota(jnp.int32, (8, INFO), 1)
    slot_lane = jnp.where(lane8 == 3 * experts + place.expert, 1.0, 0.0).astype(BF16)
    lane_t = lax.broadcasted_iota(jnp.int32, (256, INFO), 1)
    lane64 = lax.broadcasted_iota(jnp.int32, (64, INFO), 1)
    gate_lane = (lane64 % experts == place.expert) & (lane64 < 3 * experts)

    def select(source, base, chunk):
        def body(x, carry):
            g = base + x
            info = source[x, :, :, :, pl.ds(ROUTING, INFO)].reshape(256, INFO)
            code = nt_dot(slot_lane, info)[0:1]
            take = jnp.where(code == want, 1.0, 0.0).astype(BF16)
            if chunk == 0:
                code_t = jnp.sum(
                    jnp.where(lane_t == 3 * experts + place.expert, info.astype(F32), 0.0),
                    axis=1, keepdims=True,
                )
                place_t[g] = jnp.where(code_t == want_t, 1.0, 0.0).astype(BF16)
                gates = jnp.where(gate_lane, dot(take[0:64], info), 0.0)
                scale[g] = jnp.broadcast_to(jnp.sum(gates, axis=1, keepdims=True), (64, width))
            start, first_col, size = DATA[chunk]
            data = source[x, :, :, :, pl.ds(start, size)].reshape(256, size)
            rows[g, :, :, pl.ds(first_col, size)] = dot(take, data).astype(BF16).reshape(2, 64, size)
            return carry

        lax.fori_loop(0, SIDE, body, 0)

    def products(chunk, tiles):
        start, first_col, size = DATA[chunk]
        for j in tiles:
            acc = sums_gu[j] if chunk else 0.0
            for h in range(2):
                left = rows[:, h, :, pl.ds(first_col, size)].reshape(512, size)
                acc = acc + dot(left, wgu[j, pl.ds(h * HALF + first_col, size), :])
            if chunk < len(DATA) - 1:
                sums_gu[j] = acc
                continue
            v, u = acc[:, :width], acc[:, width:]
            act = v / (1.0 + jnp.exp(-v)) * u * scale[...].reshape(512, width)
            hidden[:, pl.ds(j * width, width)] = act.astype(BF16)

    select(mine, 0, 0)
    gathers[0].wait_across()
    select(other, SIDE, 0)
    gathers[2].relay3()
    for copy in loads:
        copy.wait()
    products(0, range(4))
    gathers[1].finish()
    products(0, range(4, ff_tiles))
    select(mine, 0, 1)
    gathers[2].finish()
    gathers[1].wait_across()
    select(other, SIDE, 1)
    products(1, range(ff_tiles))
    select(mine, 0, 2)
    gathers[2].wait_across()
    select(other, SIDE, 2)
    products(2, range(ff_tiles))

    def project(k):
        for h in range(2):
            y = dot(hidden[...], wd[:, pl.ds(h * HALF + k * TILE, TILE)]).astype(BF16)
            rows[:, h, :, pl.ds(k * TILE, TILE)] = y.reshape(8, 64, TILE)

    def scatter(k, target, base):
        cols = pl.ds(k * TILE, TILE)
        for x in range(SIDE):
            y = rows[base + x, :, :, cols].reshape(128, TILE)
            placed = dot(place_t[base + x], y).astype(BF16)
            target[x, :, :, :, cols] = placed.reshape(SIDE, SIDE, 16, TILE)

    def sums(part, fixed):
        return (*pick(fixed), ALL, pl.ds(part * TILE, TILE))

    def add(part, fixed, pieces):
        index = sums(part, fixed)
        total = keep[index].astype(F32)
        for ref, where in pieces:
            total = total + ref[where].astype(F32)
        keep[index] = total.astype(BF16)

    def merge(part):
        for x in range(SIDE):
            add(part, {0: x}, [(got, sums(part, {0: x}))])

    sum_base = len(GATHER) * GATHER_SEMS

    def arrival(k, what):
        return sum_base + k * SUM_SEMS + what

    def ring(k, deep):
        f1, f2, f3 = ORDERS[k % 3]
        if deep:
            return f2, f3, {f1: place.own[f1]}, relay2[k], final2[k], 6, arrival(k, 3)
        return f1, f2, {}, relay1[k], final1[k], 5, arrival(k, 1)

    def into(ref, k, dim, cut, fixed, way, h):
        axis = [d for d in range(3) if d not in fixed and d != dim].index(cut)
        index = [ALL] * (len(ref.shape) - 1)
        index[axis] = pl.ds(2 * h, 2)
        return ref.at[(way, *index)]

    def open_ring(k, deep):
        dim, cut, fixed, relays, finals, kind, base = ring(k, deep)
        for h, step in FIRST:
            src = keep.at[sums(k, {**fixed, cut: pl.ds(2 * h, 2), dim: place.at(dim, 2)})]
            send(src, relays.at[h], place.device(dim, step), kind, base)
        for way, h, step in ((0, 1, 1), (1, 0, 3)):
            src = keep.at[sums(k, {**fixed, cut: pl.ds(2 * h, 2), dim: place.at(dim, step)})]
            dst = into(finals, k, dim, cut, fixed, way, h)
            send(src, dst, place.device(dim, step), kind, base + 1)

    def pass_ring(k, deep):
        dim, cut, fixed, relays, finals, kind, base = ring(k, deep)
        arrive(relays, base)
        for h, step in FIRST:
            where = {**fixed, cut: pl.ds(2 * h, 2), dim: place.at(dim, step)}
            add(k, where, [(relays, (h,))])
            dst = into(finals, k, dim, cut, fixed, h, h)
            send(keep.at[sums(k, where)], dst, place.device(dim, step), kind, base + 1)

    def close_ring(k, deep):
        dim, cut, fixed, relays, finals, kind, base = ring(k, deep)
        arrive(finals, base + 1)
        add(k, {**fixed, dim: place.own[dim]}, [(finals, (i,)) for i in range(finals.shape[0])])

    def compute(k):
        project(k)
        scatter(k, give, SIDE)
        piece = sums(k, {})
        send(give.at[piece], got.at[piece], partner, 4, arrival(k, 0))
        scatter(k, keep, 0)

    def begin(k):
        arrive(got.at[sums(k, {})], arrival(k, 0))
        merge(k)
        open_ring(k, False)

    def pass_first(k):
        pass_ring(k, False)

    def close_first(k):
        close_ring(k, False)
        if k < DIRECT:
            open_ring(k, True)
            return
        f1, f2, f3 = ORDERS[k % 3]
        for step in (1, 3, 2):
            src = keep.at[sums(k, {f1: place.own[f1], f2: place.at(f2, step)})]
            send(src, final2[k].at[step - 1], place.device(f2, step), 6, arrival(k, 4))

    def pass_second(k):
        if k < DIRECT:
            pass_ring(k, True)

    def close_second(k):
        close_ring(k, True)
        f1, f2, f3 = ORDERS[k % 3]
        for step in (1, 3, 2):
            where = {f1: place.own[f1], f2: place.own[f2], f3: place.at(f3, step)}
            src = keep.at[sums(k, where)]
            send(src, last[k].at[step - 1], place.device(f3, step), 7, arrival(k, 5))

    def finish(k):
        arrive(last[k], arrival(k, 5))
        total = keep[sums(k, dict(enumerate(place.own)))].astype(F32)
        for i in range(3):
            total = total + last[k][i].astype(F32)
        out_ref[:, pl.ds(k * TILE, TILE)] = total[0:8].astype(BF16)
        out_ref[:, pl.ds(HALF + k * TILE, TILE)] = total[8:16].astype(BF16)

    plan = []
    for k in range(CHUNKS):
        plan.append((1.1 * k, compute, k))
        plan.append((1.1 * k + 2.25, begin, k))
        closed = 13.6 + 0.9 * k
        second = closed + (6.4 if k < DIRECT else 4.5)
        plan.append((9.3 + k, pass_first, k))
        plan.append((closed, close_first, k))
        plan.append((closed + 3.2, pass_second, k))
        plan.append((second, close_second, k))
        plan.append((second + 4.0, finish, k))
    for when, step, k in sorted(plan, key=lambda entry: entry[0]):
        step(k)

    for kind, sent in enumerate(
        (
            mine.at[pl.ds(0, 3), 0, 0], mine.at[pl.ds(0, 3), :, 0], mine.at[pl.ds(0, 3)], mine,
            keep, keep.at[pl.ds(0, 3)], keep.at[pl.ds(0, 3), :, 0], keep.at[pl.ds(0, 3), 0, 0],
        )
    ):
        waiting(sent, kind, 0).wait_send()


def ring_buffers():
    relay1, final1, relay2, final2, last = [], [], [], [], []
    for k in range(CHUNKS):
        f1, f2, f3 = ORDERS[k % 3]
        left = [d for d in range(3) if d != f1]
        relay1.append(pltpu.VMEM((2, *(2 if d == f2 else SIDE for d in left), 16, TILE), BF16))
        final1.append(pltpu.VMEM((2, SIDE, SIDE, 16, TILE), BF16))
        relay2.append(pltpu.VMEM((2, 2, 16, TILE), BF16))
        final2.append(pltpu.VMEM((2 if k < DIRECT else 3, SIDE, 16, TILE), BF16))
        last.append(pltpu.VMEM((3, 16, TILE), BF16))
    return relay1, final1, relay2, final2, last


def layer(tokens, router, expert_ids, w_gate, w_up, w_down):
    depth, ff = w_gate.shape[1], w_gate.shape[2]
    blocks = (SIDE, SIDE, SIDE, 16)
    vmem, anywhere = pl.BlockSpec(memory_space=pltpu.VMEM), pl.BlockSpec(memory_space=pl.ANY)
    return pl.pallas_call(
        layer_kernel,
        out_shape=jax.ShapeDtypeStruct(tokens.shape, BF16),
        in_specs=[vmem, vmem, vmem, anywhere, anywhere, anywhere],
        out_specs=vmem,
        scratch_shapes=[
            pltpu.VMEM((ff // (TILE // 2), depth, TILE), BF16),
            pltpu.VMEM((ff, depth), BF16),
            pltpu.VMEM((*blocks, HALF + INFO), BF16),
            pltpu.VMEM((*blocks, HALF + INFO), BF16),
            pltpu.VMEM((8, 2, 64, HALF), BF16),
            pltpu.VMEM((8, 64, TILE // 2), F32),
            pltpu.VMEM((8, 256, 128), BF16),
            pltpu.VMEM((ff // (TILE // 2), 512, TILE), F32),
            pltpu.VMEM((512, ff), BF16),
            pltpu.VMEM((*blocks, HALF), BF16),
            pltpu.VMEM((*blocks, HALF), BF16),
            pltpu.VMEM((*blocks, HALF), BF16),
            *ring_buffers(),
            pltpu.SemaphoreType.DMA((2 * (ff // (TILE // 2)) + 1,)),
            pltpu.SemaphoreType.DMA((8,)),
            pltpu.SemaphoreType.DMA((len(GATHER) * GATHER_SEMS + CHUNKS * SUM_SEMS,)),
        ],
        compiler_params=pltpu.CompilerParams(
            collective_id=0, has_side_effects=True, vmem_limit_bytes=67043328
        ),
    )(tokens, router.T, expert_ids.T, w_gate, w_up, w_down)


def solution(mesh):
    placed = (
        P(("expert", "shard"), None),
        P(),
        P(("expert", "shard"), None),
        P("expert", None, "shard"),
        P("expert", None, "shard"),
        P("expert", "shard", None),
    )
    return jax.shard_map(
        layer, mesh=mesh, in_specs=placed, out_specs=P(("expert", "shard"), None), check_vma=False
    )
```

```python
import functools

import jax
import jax.numpy as jnp
from jax import lax
from jax.experimental import pallas as pl
from jax.experimental.pallas import tpu as pltpu
from jax.sharding import PartitionSpec as P

MESH = pl.DeviceIdType.MESH
BF16, F32 = jnp.bfloat16, jnp.float32
ALL = slice(None)
FIRST, SECOND = ((0, 1), (1, 3)), ((1, 1), (0, 3))
AROUND = (1, 3, 2)

SIDE = 4
HALF = 2048
INFO = 128
DATA = ((0, 0, 768), (768 + INFO, 768, 768), (1536 + INFO, 1536, 512))
ROUTING = 768
GATHER = (
    ((0, 256), (256, 256), (512, 256 + INFO)),
    ((896, 256), (1152, 256), (1408, 256)),
    ((1664, 256), (1920, 256)),
)
ORDERS = ((0, 1, 2), (1, 2, 0), (2, 0, 1))
TILE = 256
CHUNKS = HALF // TILE
DIRECT = 5
GATHER_SEMS, SUM_SEMS = 16, 6


def nt_dot(a, b):
    return lax.dot_general(a, b, (((1,), (1,)), ((), ())), preferred_element_type=F32)


def dot(a, b):
    return jnp.dot(a, b, preferred_element_type=F32)


class Place:
    def __init__(self):
        expert, shard = lax.axis_index("expert"), lax.axis_index("shard")
        self.expert = expert
        self.core = expert % 2
        self.own = (expert // 2, shard // SIDE, shard % SIDE)

    def device(self, dim=None, step=0, core=None):
        x, z, y = (
            lax.rem(v + step, SIDE) if d == dim else v for d, v in enumerate(self.own)
        )
        return (x * 2 + (self.core if core is None else core), z * SIDE + y)

    def at(self, dim, step):
        return lax.rem(self.own[dim] + step, SIDE)


def pick(fixed):
    return tuple(fixed.get(d, ALL) for d in range(3))


def routing_info(place, tok, ids, router_t):
    logits = nt_dot(tok, router_t)
    experts = logits.shape[1]
    small = lax.broadcasted_iota(jnp.int32, logits.shape, 1)
    same = small == lax.broadcasted_iota(jnp.int32, logits.shape, 0)
    id0, id1 = [
        jnp.sum(jnp.where(same, ids[k : k + 1, :], 0), axis=1, keepdims=True) for k in range(2)
    ]
    chosen = [jnp.sum(jnp.where(small == i, logits, 0.0), axis=1, keepdims=True) for i in (id0, id1)]
    first = 1.0 / (1.0 + jnp.exp(-(chosen[0] - chosen[1])))
    rows = tok.shape[0]
    lane = lax.broadcasted_iota(jnp.int32, (rows, INFO), 1)
    section, of = lane // experts, lane % experts
    is0, is1 = of == id0, of == id1
    gate = jnp.where(is0, first, jnp.where(is1, 1.0 - first, 0.0))
    named = jnp.where(is0 | is1, 1.0, 0.0)
    lower = lax.broadcasted_iota(jnp.int32, (rows, rows), 0) > lax.broadcasted_iota(
        jnp.int32, (rows, rows), 1
    )
    before = dot(jnp.where(lower, 1.0, 0.0).astype(BF16), named.astype(BF16))
    top = gate.astype(BF16).astype(F32)
    middle = (gate - top).astype(BF16).astype(F32)
    low = gate - top - middle
    info = jnp.where(section == 0, top, jnp.where(section == 1, middle, low))
    info = jnp.where(section == 3, named * (before + 1.0), info)
    return jnp.where(section > 3, 0.0, info)


def layer_kernel(
    tok_ref, router_ref, ids_ref, gate_hbm, up_hbm, down_hbm, out_ref,
    wgu, wd, mine, other, rows, scale, take, place_t, sums_gu, hidden, keep, give, got,
    relay1, final1, relay2, final2, last, w_sems, send_sems, recv_sems,
):
    place = Place()
    experts = router_ref.shape[0]
    ff_tiles = wgu.shape[0]
    width = TILE // 2

    loads = []
    for j in range(ff_tiles):
        span = pl.ds(j * width, width)
        loads.append((gate_hbm.at[0, :, span], wgu.at[j, :, pl.ds(0, width)]))
        loads.append((up_hbm.at[0, :, span], wgu.at[j, :, pl.ds(width, width)]))
    loads.append((down_hbm.at[0], wd))
    loads = [pltpu.make_async_copy(s, d, w_sems.at[i]) for i, (s, d) in enumerate(loads)]
    for copy in loads:
        copy.start()

    barrier = pltpu.get_barrier_semaphore()
    partners = [place.device(d, step) for d in range(3) for step in (1, 2, 3)]
    partners.append(place.device(core=1 - place.core))
    for partner in partners:
        pl.semaphore_signal(barrier, inc=1, device_id=partner, device_id_type=MESH)

    tok = tok_ref[...]
    block = jnp.concatenate([tok[:, :HALF].astype(F32), tok[:, HALF:].astype(F32)], axis=0)
    info = routing_info(place, tok, ids_ref[...], router_ref[...])
    block = block.astype(BF16)
    for start, first_col, size in DATA:
        mine[(*place.own, ALL, pl.ds(start, size))] = block[:, first_col : first_col + size]
    mine[(*place.own, ALL, pl.ds(ROUTING, INFO))] = jnp.concatenate([info, info], axis=0).astype(BF16)
    pl.semaphore_wait(barrier, len(partners))

    def send(src, dst, device, kind, arrival):
        pltpu.make_async_remote_copy(
            src_ref=src, dst_ref=dst, send_sem=send_sems.at[kind], recv_sem=recv_sems.at[arrival],
            device_id=device, device_id_type=MESH,
        ).start()

    def waiting(ref, kind, arrival):
        return pltpu.make_async_remote_copy(
            src_ref=ref, dst_ref=ref, send_sem=send_sems.at[kind], recv_sem=recv_sems.at[arrival],
            device_id=partner, device_id_type=MESH,
        )

    def arrive(ref, arrival):
        waiting(ref, 0, arrival).wait_recv()

    partner = place.device(core=1 - place.core)

    def block_slice(ref, chunk, part, fixed):
        return ref.at[(*pick(fixed), ALL, pl.ds(*GATHER[chunk][part]))]

    class Gather:
        def __init__(self, chunk):
            self.chunk, self.parts = chunk, range(len(GATHER[chunk]))
            self.base = chunk * GATHER_SEMS
            start = GATHER[chunk][0][0]
            self.cols = pl.ds(start, sum(size for _, size in GATHER[chunk]))
            for part in self.parts:
                piece = block_slice(mine, chunk, part, dict(enumerate(place.own)))
                for step in (1, 2, 3):
                    send(piece, piece, place.device(ORDERS[part][0], step), 0, self.base)

        def whole(self, fixed):
            return mine.at[(*pick(fixed), ALL, self.cols)]

        def pieces(self, part, fixed, dim, offset, ways, kind, arrival):
            for h, step in ways:
                where = {**fixed, ORDERS[part][0]: pl.ds(2 * h, 2), dim: place.at(dim, offset(step))}
                piece = block_slice(mine, self.chunk, part, where)
                send(piece, piece, place.device(dim, step), kind, arrival)

        def level(self, part, deep, at2):
            d1, d2, d3 = ORDERS[part]
            if deep:
                return [({d2: place.at(d2, o)}, d3, 2) for o in at2]
            return [({d3: place.own[d3]}, d2, 1)]

        def spread(self, part, deep, ways, arrival, at2=()):
            for fixed, dim, kind in self.level(part, deep, at2):
                self.pieces(part, fixed, dim, lambda step: 0, ways, kind, self.base + arrival)

        def relay(self, part, deep, arrival, at2=()):
            for fixed, dim, kind in self.level(part, deep, at2):
                self.pieces(
                    part, fixed, dim, lambda step: 4 - step, FIRST, kind, self.base + arrival
                )

        def to_partner(self, step):
            for part in self.parts:
                dim = ORDERS[part][2]
                where = {dim: place.at(dim, step)}
                src = block_slice(mine, self.chunk, part, where)
                dst = block_slice(other, self.chunk, part, where)
                send(src, dst, partner, 3, self.base + 12)

        def spread2(self):
            arrive(self.whole({0: pl.ds(0, 3), 1: 0, 2: 0}), self.base)
            for part in self.parts:
                self.spread(part, False, FIRST, 1 + part)
                self.spread(part, False, SECOND, 4 + part)

        def early3(self):
            for part in self.parts:
                self.spread(part, True, FIRST, 13 + part, (0,))
                self.spread(part, True, SECOND, 10, (0,))

        def four(self, part):
            d1, d2, d3 = ORDERS[part]
            return block_slice(mine, self.chunk, part, {d2: place.own[d2], d3: place.own[d3]})

        def relay2(self):
            for part in self.parts:
                arrive(self.four(part), self.base + 1 + part)
                self.relay(part, False, 4 + part)

        def relay3_early(self):
            for part in self.parts:
                arrive(self.four(part), self.base + 13 + part)
                self.relay(part, True, 11, (0,))

        def spread3_first(self):
            for part in self.parts:
                d1, d2, d3 = ORDERS[part]
                where = {d2: pl.ds(0, 2), d3: place.own[d3]}
                arrive(block_slice(mine, self.chunk, part, where), self.base + 4 + part)
                self.spread(part, True, FIRST, 7 + part, AROUND)

        def spread3_second(self):
            for part in self.parts:
                self.spread(part, True, SECOND, 10, AROUND)
            self.to_partner(0)

        def relay3(self):
            for part in self.parts:
                d1, d2, d3 = ORDERS[part]
                where = {d2: pl.ds(0, 3), d3: place.own[d3]}
                arrive(block_slice(mine, self.chunk, part, where), self.base + 7 + part)
                self.relay(part, True, 11, AROUND)

        def finish(self):
            arrive(self.whole({0: 0}), self.base + 10)
            self.to_partner(1)
            self.to_partner(3)
            arrive(self.whole({0: 0}), self.base + 11)
            self.to_partner(2)

        def wait_across(self):
            arrive(self.whole({}), self.base + 12)

    gathers = [Gather(chunk) for chunk in range(len(GATHER))]
    for g in gathers:
        g.spread2()
    for g in gathers:
        g.early3()
    for g in gathers:
        g.relay2()
    for g in gathers:
        g.relay3_early()
    gathers[0].spread3_first()
    gathers[0].spread3_second()
    gathers[1].spread3_first()
    gathers[0].relay3()
    gathers[1].spread3_second()
    gathers[2].spread3_first()
    gathers[1].relay3()
    gathers[2].spread3_second()
    gathers[0].finish()

    r_i = lax.broadcasted_iota(jnp.int32, (128, 256), 0)
    c_i = lax.broadcasted_iota(jnp.int32, (128, 256), 1)
    fits = (c_i // 16 == (r_i % 64) // 4) & ((c_i // 8) % 2 == r_i // 64)
    want = jnp.where(fits, r_i % 4 + 1, -1).astype(F32)
    c_t = lax.broadcasted_iota(jnp.int32, (256, 128), 0)
    r_t = lax.broadcasted_iota(jnp.int32, (256, 128), 1)
    fits_t = (c_t // 16 == (r_t % 64) // 4) & ((c_t // 8) % 2 == r_t // 64)
    want_t = jnp.where(fits_t, r_t % 4 + 1, -1).astype(F32)
    lane8 = lax.broadcasted_iota(jnp.int32, (8, INFO), 1)
    slot_lane = jnp.where(lane8 == 3 * experts + place.expert, 1.0, 0.0).astype(BF16)
    lane_t = lax.broadcasted_iota(jnp.int32, (256, INFO), 1)
    lane64 = lax.broadcasted_iota(jnp.int32, (64, INFO), 1)
    gate_lane = (lane64 % experts == place.expert) & (lane64 < 3 * experts)

    def route(source, base):
        for x in range(SIDE):
            g = base + x
            info = source[x, :, :, :, pl.ds(ROUTING, INFO)].reshape(256, INFO)
            code = nt_dot(slot_lane, info)[0:1]
            take[g] = jnp.where(code == want, 1.0, 0.0).astype(BF16)

    def route_back(source, base):
        for x in range(SIDE):
            g = base + x
            info = source[x, :, :, :, pl.ds(ROUTING, INFO)].reshape(256, INFO)
            code_t = jnp.sum(
                jnp.where(lane_t == 3 * experts + place.expert, info.astype(F32), 0.0),
                axis=1, keepdims=True,
            )
            place_t[g] = jnp.where(code_t == want_t, 1.0, 0.0).astype(BF16)
            gates = jnp.where(gate_lane, dot(take[g, pl.ds(0, 64)], info), 0.0)
            scale[g] = jnp.broadcast_to(jnp.sum(gates, axis=1, keepdims=True), (64, width))

    def select(source, base, chunk):
        start, first_col, size = DATA[chunk]
        for x in range(SIDE):
            data = source[x, :, :, :, pl.ds(start, size)].reshape(256, size)
            chosen = dot(take[base + x], data).astype(BF16).reshape(2, 64, size)
            rows[base + x, :, :, pl.ds(first_col, size)] = chosen

    def products(chunk, tiles):
        start, first_col, size = DATA[chunk]
        for j in tiles:
            acc = sums_gu[j] if chunk else 0.0
            for h in range(2):
                left = rows[:, h, :, pl.ds(first_col, size)].reshape(512, size)
                acc = acc + dot(left, wgu[j, pl.ds(h * HALF + first_col, size), :])
            if chunk < len(DATA) - 1:
                sums_gu[j] = acc
                continue
            v, u = acc[:, :width], acc[:, width:]
            act = v / (1.0 + jnp.exp(-v)) * u * scale[...].reshape(512, width)
            hidden[:, pl.ds(j * width, width)] = act.astype(BF16)

    gathers[2].relay3()
    route(mine, 0)
    select(mine, 0, 0)
    route_back(mine, 0)
    gathers[0].wait_across()
    route(other, SIDE)
    select(other, SIDE, 0)
    for copy in loads:
        copy.wait()
    products(0, range(4))
    gathers[1].finish()
    products(0, range(4, ff_tiles))
    gathers[2].finish()
    select(mine, 0, 1)
    route_back(other, SIDE)
    gathers[1].wait_across()
    select(other, SIDE, 1)
    select(mine, 0, 2)
    products(1, range(ff_tiles))
    gathers[2].wait_across()
    select(other, SIDE, 2)
    products(2, range(ff_tiles))

    def project(k):
        for h in range(2):
            y = dot(hidden[...], wd[:, pl.ds(h * HALF + k * TILE, TILE)]).astype(BF16)
            rows[:, h, :, pl.ds(k * TILE, TILE)] = y.reshape(8, 64, TILE)

    def scatter(k, target, base):
        cols = pl.ds(k * TILE, TILE)
        for x in range(SIDE):
            y = rows[base + x, :, :, cols].reshape(128, TILE)
            placed = dot(place_t[base + x], y).astype(BF16)
            target[x, :, :, :, cols] = placed.reshape(SIDE, SIDE, 16, TILE)

    def sums(part, fixed):
        return (*pick(fixed), ALL, pl.ds(part * TILE, TILE))

    def add(part, fixed, pieces):
        index = sums(part, fixed)
        total = keep[index].astype(F32)
        for ref, where in pieces:
            total = total + ref[where].astype(F32)
        keep[index] = total.astype(BF16)

    def merge(part):
        for x in range(SIDE):
            add(part, {0: x}, [(got, sums(part, {0: x}))])

    sum_base = len(GATHER) * GATHER_SEMS

    def arrival(k, what):
        return sum_base + k * SUM_SEMS + what

    def ring(k, deep):
        f1, f2, f3 = ORDERS[k % 3]
        if deep:
            return f2, f3, {f1: place.own[f1]}, relay2[k], final2[k], 6, arrival(k, 3)
        return f1, f2, {}, relay1[k], final1[k], 5, arrival(k, 1)

    def into(ref, k, dim, cut, fixed, way, h):
        axis = [d for d in range(3) if d not in fixed and d != dim].index(cut)
        index = [ALL] * (len(ref.shape) - 1)
        index[axis] = pl.ds(2 * h, 2)
        return ref.at[(way, *index)]

    def open_ring(k, deep):
        dim, cut, fixed, relays, finals, kind, base = ring(k, deep)
        for h, step in FIRST:
            src = keep.at[sums(k, {**fixed, cut: pl.ds(2 * h, 2), dim: place.at(dim, 2)})]
            send(src, relays.at[h], place.device(dim, step), kind, base)
        for way, h, step in ((0, 1, 1), (1, 0, 3)):
            src = keep.at[sums(k, {**fixed, cut: pl.ds(2 * h, 2), dim: place.at(dim, step)})]
            dst = into(finals, k, dim, cut, fixed, way, h)
            send(src, dst, place.device(dim, step), kind, base + 1)

    def pass_ring(k, deep):
        dim, cut, fixed, relays, finals, kind, base = ring(k, deep)
        arrive(relays, base)
        for h, step in FIRST:
            where = {**fixed, cut: pl.ds(2 * h, 2), dim: place.at(dim, step)}
            add(k, where, [(relays, (h,))])
            dst = into(finals, k, dim, cut, fixed, h, h)
            send(keep.at[sums(k, where)], dst, place.device(dim, step), kind, base + 1)

    def close_ring(k, deep):
        dim, cut, fixed, relays, finals, kind, base = ring(k, deep)
        arrive(finals, base + 1)
        add(k, {**fixed, dim: place.own[dim]}, [(finals, (i,)) for i in range(finals.shape[0])])

    def compute(k):
        project(k)
        scatter(k, give, SIDE)
        piece = sums(k, {})
        send(give.at[piece], got.at[piece], partner, 4, arrival(k, 0))
        scatter(k, keep, 0)

    def begin(k):
        arrive(got.at[sums(k, {})], arrival(k, 0))
        merge(k)
        open_ring(k, False)

    def pass_first(k):
        pass_ring(k, False)

    def close_first(k):
        close_ring(k, False)
        if k < DIRECT:
            open_ring(k, True)
            return
        f1, f2, f3 = ORDERS[k % 3]
        for step in (1, 3, 2):
            src = keep.at[sums(k, {f1: place.own[f1], f2: place.at(f2, step)})]
            send(src, final2[k].at[step - 1], place.device(f2, step), 6, arrival(k, 4))

    def pass_second(k):
        if k < DIRECT:
            pass_ring(k, True)

    def close_second(k):
        close_ring(k, True)
        f1, f2, f3 = ORDERS[k % 3]
        for step in (1, 3, 2):
            where = {f1: place.own[f1], f2: place.own[f2], f3: place.at(f3, step)}
            src = keep.at[sums(k, where)]
            send(src, last[k].at[step - 1], place.device(f3, step), 7, arrival(k, 5))

    def finish(k):
        arrive(last[k], arrival(k, 5))
        total = keep[sums(k, dict(enumerate(place.own)))].astype(F32)
        for i in range(3):
            total = total + last[k][i].astype(F32)
        out_ref[:, pl.ds(k * TILE, TILE)] = total[0:8].astype(BF16)
        out_ref[:, pl.ds(HALF + k * TILE, TILE)] = total[8:16].astype(BF16)

    plan = []
    for k in range(CHUNKS):
        plan.append((1.1 * k, compute, k))
        plan.append((1.1 * k + 2.25, begin, k))
        closed = 13.6 + 0.9 * k
        second = closed + (6.4 if k < DIRECT else 4.5)
        plan.append((7.3 + k, pass_first, k))
        plan.append((closed, close_first, k))
        plan.append((closed + 3.2, pass_second, k))
        plan.append((second, close_second, k))
        plan.append((second + 4.0, finish, k))
    for when, step, k in sorted(plan, key=lambda entry: entry[0]):
        step(k)

    for kind, sent in enumerate(
        (
            mine.at[pl.ds(0, 3), 0, 0], mine.at[pl.ds(0, 3), :, 0], mine.at[pl.ds(0, 3)], mine,
            keep, keep.at[pl.ds(0, 3)], keep.at[pl.ds(0, 3), :, 0], keep.at[pl.ds(0, 3), 0, 0],
        )
    ):
        waiting(sent, kind, 0).wait_send()


def ring_buffers():
    relay1, final1, relay2, final2, last = [], [], [], [], []
    for k in range(CHUNKS):
        f1, f2, f3 = ORDERS[k % 3]
        left = [d for d in range(3) if d != f1]
        relay1.append(pltpu.VMEM((2, *(2 if d == f2 else SIDE for d in left), 16, TILE), BF16))
        final1.append(pltpu.VMEM((2, SIDE, SIDE, 16, TILE), BF16))
        relay2.append(pltpu.VMEM((2, 2, 16, TILE), BF16))
        final2.append(pltpu.VMEM((2 if k < DIRECT else 3, SIDE, 16, TILE), BF16))
        last.append(pltpu.VMEM((3, 16, TILE), BF16))
    return relay1, final1, relay2, final2, last


def layer(tokens, router, expert_ids, w_gate, w_up, w_down):
    depth, ff = w_gate.shape[1], w_gate.shape[2]
    blocks = (SIDE, SIDE, SIDE, 16)
    vmem, anywhere = pl.BlockSpec(memory_space=pltpu.VMEM), pl.BlockSpec(memory_space=pl.ANY)
    return pl.pallas_call(
        layer_kernel,
        out_shape=jax.ShapeDtypeStruct(tokens.shape, BF16),
        in_specs=[vmem, vmem, vmem, anywhere, anywhere, anywhere],
        out_specs=vmem,
        scratch_shapes=[
            pltpu.VMEM((ff // (TILE // 2), depth, TILE), BF16),
            pltpu.VMEM((ff, depth), BF16),
            pltpu.VMEM((*blocks, HALF + INFO), BF16),
            pltpu.VMEM((*blocks, HALF + INFO), BF16),
            pltpu.VMEM((8, 2, 64, HALF), BF16),
            pltpu.VMEM((8, 64, TILE // 2), F32),
            pltpu.VMEM((8, 128, 256), BF16),
            pltpu.VMEM((8, 256, 128), BF16),
            pltpu.VMEM((ff // (TILE // 2), 512, TILE), F32),
            pltpu.VMEM((512, ff), BF16),
            pltpu.VMEM((*blocks, HALF), BF16),
            pltpu.VMEM((*blocks, HALF), BF16),
            pltpu.VMEM((*blocks, HALF), BF16),
            *ring_buffers(),
            pltpu.SemaphoreType.DMA((2 * (ff // (TILE // 2)) + 1,)),
            pltpu.SemaphoreType.DMA((8,)),
            pltpu.SemaphoreType.DMA((len(GATHER) * GATHER_SEMS + CHUNKS * SUM_SEMS,)),
        ],
        compiler_params=pltpu.CompilerParams(
            collective_id=0, has_side_effects=True, vmem_limit_bytes=67043328
        ),
    )(tokens, router.T, expert_ids.T, w_gate, w_up, w_down)


def solution(mesh):
    placed = (
        P(("expert", "shard"), None),
        P(),
        P(("expert", "shard"), None),
        P("expert", None, "shard"),
        P("expert", None, "shard"),
        P("expert", "shard", None),
    )
    return jax.shard_map(
        layer, mesh=mesh, in_specs=placed, out_specs=P(("expert", "shard"), None), check_vma=False
    )
```

```python
import functools

import jax
import jax.numpy as jnp
from jax import lax
from jax.experimental import pallas as pl
from jax.experimental.pallas import tpu as pltpu
from jax.sharding import PartitionSpec as P

MESH = pl.DeviceIdType.MESH
BF16, F32 = jnp.bfloat16, jnp.float32
ALL = slice(None)
FIRST, SECOND = ((0, 1), (1, 3)), ((1, 1), (0, 3))
AROUND = (1, 3, 2)

SIDE = 4
HALF = 2048
INFO = 128
DATA = ((0, 0, 768), (768 + INFO, 768, 768), (1536 + INFO, 1536, 512))
ROUTING = 768
GATHER = (
    ((0, 256), (256, 256), (512, 256 + INFO)),
    ((896, 256), (1152, 256), (1408, 256)),
    ((1664, 256), (1920, 256)),
)
ORDERS = ((0, 1, 2), (1, 2, 0), (2, 0, 1))
TILE = 256
CHUNKS = HALF // TILE
DIRECT = 5
GATHER_SEMS, SUM_SEMS = 16, 8


def nt_dot(a, b):
    return lax.dot_general(a, b, (((1,), (1,)), ((), ())), preferred_element_type=F32)


def dot(a, b):
    return jnp.dot(a, b, preferred_element_type=F32)


class Place:
    def __init__(self):
        expert, shard = lax.axis_index("expert"), lax.axis_index("shard")
        self.expert = expert
        self.core = expert % 2
        self.own = (expert // 2, shard // SIDE, shard % SIDE)

    def device(self, dim=None, step=0, core=None):
        x, z, y = (
            lax.rem(v + step, SIDE) if d == dim else v for d, v in enumerate(self.own)
        )
        return (x * 2 + (self.core if core is None else core), z * SIDE + y)

    def at(self, dim, step):
        return lax.rem(self.own[dim] + step, SIDE)


def pick(fixed):
    return tuple(fixed.get(d, ALL) for d in range(3))


def routing_info(place, tok, ids, router_t):
    logits = nt_dot(tok, router_t)
    experts = logits.shape[1]
    small = lax.broadcasted_iota(jnp.int32, logits.shape, 1)
    same = small == lax.broadcasted_iota(jnp.int32, logits.shape, 0)
    id0, id1 = [
        jnp.sum(jnp.where(same, ids[k : k + 1, :], 0), axis=1, keepdims=True) for k in range(2)
    ]
    chosen = [jnp.sum(jnp.where(small == i, logits, 0.0), axis=1, keepdims=True) for i in (id0, id1)]
    first = 1.0 / (1.0 + jnp.exp(-(chosen[0] - chosen[1])))
    rows = tok.shape[0]
    lane = lax.broadcasted_iota(jnp.int32, (rows, INFO), 1)
    section, of = lane // experts, lane % experts
    is0, is1 = of == id0, of == id1
    gate = jnp.where(is0, first, jnp.where(is1, 1.0 - first, 0.0))
    named = jnp.where(is0 | is1, 1.0, 0.0)
    lower = lax.broadcasted_iota(jnp.int32, (rows, rows), 0) > lax.broadcasted_iota(
        jnp.int32, (rows, rows), 1
    )
    before = dot(jnp.where(lower, 1.0, 0.0).astype(BF16), named.astype(BF16))
    top = gate.astype(BF16).astype(F32)
    middle = (gate - top).astype(BF16).astype(F32)
    low = gate - top - middle
    info = jnp.where(section == 0, top, jnp.where(section == 1, middle, low))
    info = jnp.where(section == 3, named * (before + 1.0), info)
    return jnp.where(section > 3, 0.0, info)


def layer_kernel(
    tok_hbm, router_hbm, ids_hbm, gate_hbm, up_hbm, down_hbm, out_hbm,
    tok_ref, router_ref, ids_ref, out_ref,
    wgu, wd, mine, other, rows, scale, take, place_t, sums_gu, hidden, keep, give, got,
    relay1, final1, relay2, final2, last, in_sems, w_sems, send_sems, recv_sems,
):
    place = Place()
    experts = router_ref.shape[0]
    ff_tiles = wgu.shape[0]
    width = TILE // 2

    inputs = [
        pltpu.make_async_copy(src, dst, in_sems.at[i])
        for i, (src, dst) in enumerate(
            ((tok_hbm, tok_ref), (ids_hbm, ids_ref), (router_hbm, router_ref))
        )
    ]
    for copy in inputs:
        copy.start()

    barrier = pltpu.get_barrier_semaphore()
    partners = [place.device(d, step) for d in range(3) for step in (1, 2, 3)]
    partners.append(place.device(core=1 - place.core))
    for partner in partners:
        pl.semaphore_signal(barrier, inc=1, device_id=partner, device_id_type=MESH)

    loads = []
    for j in range(ff_tiles):
        span = pl.ds(j * width, width)
        loads.append((gate_hbm.at[0, :, span], wgu.at[j, :, pl.ds(0, width)]))
        loads.append((up_hbm.at[0, :, span], wgu.at[j, :, pl.ds(width, width)]))
    loads.append((down_hbm.at[0], wd))
    loads = [pltpu.make_async_copy(s, d, w_sems.at[i]) for i, (s, d) in enumerate(loads)]
    for copy in loads:
        copy.start()

    for copy in inputs:
        copy.wait()
    tok = tok_ref[...]
    block = jnp.concatenate([tok[:, :HALF].astype(F32), tok[:, HALF:].astype(F32)], axis=0)
    info = routing_info(place, tok, ids_ref[...], router_ref[...])
    block = block.astype(BF16)
    for start, first_col, size in DATA:
        mine[(*place.own, ALL, pl.ds(start, size))] = block[:, first_col : first_col + size]
    mine[(*place.own, ALL, pl.ds(ROUTING, INFO))] = jnp.concatenate([info, info], axis=0).astype(BF16)
    pl.semaphore_wait(barrier, len(partners))

    def send(src, dst, device, kind, arrival):
        pltpu.make_async_remote_copy(
            src_ref=src, dst_ref=dst, send_sem=send_sems.at[kind], recv_sem=recv_sems.at[arrival],
            device_id=device, device_id_type=MESH,
        ).start()

    def waiting(ref, kind, arrival):
        return pltpu.make_async_remote_copy(
            src_ref=ref, dst_ref=ref, send_sem=send_sems.at[kind], recv_sem=recv_sems.at[arrival],
            device_id=partner, device_id_type=MESH,
        )

    def arrive(ref, arrival):
        waiting(ref, 0, arrival).wait_recv()

    partner = place.device(core=1 - place.core)

    def block_slice(ref, chunk, part, fixed):
        return ref.at[(*pick(fixed), ALL, pl.ds(*GATHER[chunk][part]))]

    class Gather:
        def __init__(self, chunk):
            self.chunk, self.parts = chunk, range(len(GATHER[chunk]))
            self.base = chunk * GATHER_SEMS
            start = GATHER[chunk][0][0]
            self.cols = pl.ds(start, sum(size for _, size in GATHER[chunk]))
            for part in self.parts:
                piece = block_slice(mine, chunk, part, dict(enumerate(place.own)))
                for step in (1, 2, 3):
                    send(piece, piece, place.device(ORDERS[part][0], step), 0, self.base)

        def whole(self, fixed):
            return mine.at[(*pick(fixed), ALL, self.cols)]

        def pieces(self, part, fixed, dim, offset, ways, kind, arrival):
            for h, step in ways:
                where = {**fixed, ORDERS[part][0]: pl.ds(2 * h, 2), dim: place.at(dim, offset(step))}
                piece = block_slice(mine, self.chunk, part, where)
                send(piece, piece, place.device(dim, step), kind, arrival)

        def level(self, part, deep, at2):
            d1, d2, d3 = ORDERS[part]
            if deep:
                return [({d2: place.at(d2, o)}, d3, 2) for o in at2]
            return [({d3: place.own[d3]}, d2, 1)]

        def spread(self, part, deep, ways, arrival, at2=()):
            for fixed, dim, kind in self.level(part, deep, at2):
                self.pieces(part, fixed, dim, lambda step: 0, ways, kind, self.base + arrival)

        def relay(self, part, deep, arrival, at2=()):
            for fixed, dim, kind in self.level(part, deep, at2):
                self.pieces(
                    part, fixed, dim, lambda step: 4 - step, FIRST, kind, self.base + arrival
                )

        def to_partner(self, step):
            for part in self.parts:
                dim = ORDERS[part][2]
                where = {dim: place.at(dim, step)}
                src = block_slice(mine, self.chunk, part, where)
                dst = block_slice(other, self.chunk, part, where)
                send(src, dst, partner, 3, self.base + 12)

        def spread2(self):
            arrive(self.whole({0: pl.ds(0, 3), 1: 0, 2: 0}), self.base)
            for part in self.parts:
                self.spread(part, False, FIRST, 1 + part)
                self.spread(part, False, SECOND, 4 + part)

        def early3(self):
            for part in self.parts:
                self.spread(part, True, FIRST, 13 + part, (0,))
                self.spread(part, True, SECOND, 10, (0,))

        def four(self, part):
            d1, d2, d3 = ORDERS[part]
            return block_slice(mine, self.chunk, part, {d2: place.own[d2], d3: place.own[d3]})

        def relay2(self):
            for part in self.parts:
                arrive(self.four(part), self.base + 1 + part)
                self.relay(part, False, 4 + part)

        def relay3_early(self):
            for part in self.parts:
                arrive(self.four(part), self.base + 13 + part)
                self.relay(part, True, 11, (0,))

        def spread3_first(self):
            for part in self.parts:
                d1, d2, d3 = ORDERS[part]
                where = {d2: pl.ds(0, 2), d3: place.own[d3]}
                arrive(block_slice(mine, self.chunk, part, where), self.base + 4 + part)
                self.spread(part, True, FIRST, 7 + part, AROUND)

        def spread3_second(self):
            for part in self.parts:
                self.spread(part, True, SECOND, 10, AROUND)
            self.to_partner(0)

        def relay3(self):
            for part in self.parts:
                d1, d2, d3 = ORDERS[part]
                where = {d2: pl.ds(0, 3), d3: place.own[d3]}
                arrive(block_slice(mine, self.chunk, part, where), self.base + 7 + part)
                self.relay(part, True, 11, AROUND)

        def finish(self):
            arrive(self.whole({0: 0}), self.base + 10)
            self.to_partner(1)
            self.to_partner(3)
            arrive(self.whole({0: 0}), self.base + 11)
            self.to_partner(2)

        def wait_across(self):
            arrive(self.whole({}), self.base + 12)

    gathers = [Gather(chunk) for chunk in range(len(GATHER))]
    for g in gathers:
        g.spread2()
    for g in gathers:
        g.early3()
    for g in gathers:
        g.relay2()
    for g in gathers:
        g.relay3_early()
    gathers[0].spread3_first()
    gathers[0].spread3_second()
    gathers[1].spread3_first()
    gathers[0].relay3()
    gathers[1].spread3_second()
    gathers[2].spread3_first()
    gathers[1].relay3()
    gathers[2].spread3_second()
    gathers[0].finish()

    r_i = lax.broadcasted_iota(jnp.int32, (128, 256), 0)
    c_i = lax.broadcasted_iota(jnp.int32, (128, 256), 1)
    fits = (c_i // 16 == (r_i % 64) // 4) & ((c_i // 8) % 2 == r_i // 64)
    want = jnp.where(fits, r_i % 4 + 1, -1).astype(F32)
    c_t = lax.broadcasted_iota(jnp.int32, (256, 128), 0)
    r_t = lax.broadcasted_iota(jnp.int32, (256, 128), 1)
    fits_t = (c_t // 16 == (r_t % 64) // 4) & ((c_t // 8) % 2 == r_t // 64)
    want_t = jnp.where(fits_t, r_t % 4 + 1, -1).astype(F32)
    lane8 = lax.broadcasted_iota(jnp.int32, (8, INFO), 1)
    slot_lane = jnp.where(lane8 == 3 * experts + place.expert, 1.0, 0.0).astype(BF16)
    lane_t = lax.broadcasted_iota(jnp.int32, (256, INFO), 1)
    lane64 = lax.broadcasted_iota(jnp.int32, (64, INFO), 1)
    gate_lane = (lane64 % experts == place.expert) & (lane64 < 3 * experts)

    def route(source, base):
        for x in range(SIDE):
            g = base + x
            info = source[x, :, :, :, pl.ds(ROUTING, INFO)].reshape(256, INFO)
            code = nt_dot(slot_lane, info)[0:1]
            take[g] = jnp.where(code == want, 1.0, 0.0).astype(BF16)

    def route_back(source, base):
        for x in range(SIDE):
            g = base + x
            info = source[x, :, :, :, pl.ds(ROUTING, INFO)].reshape(256, INFO)
            code_t = jnp.sum(
                jnp.where(lane_t == 3 * experts + place.expert, info.astype(F32), 0.0),
                axis=1, keepdims=True,
            )
            place_t[g] = jnp.where(code_t == want_t, 1.0, 0.0).astype(BF16)
            gates = jnp.where(gate_lane, dot(take[g, pl.ds(0, 64)], info), 0.0)
            scale[g] = jnp.broadcast_to(jnp.sum(gates, axis=1, keepdims=True), (64, width))

    def select(source, base, chunk):
        start, first_col, size = DATA[chunk]
        for x in range(SIDE):
            data = source[x, :, :, :, pl.ds(start, size)].reshape(256, size)
            chosen = dot(take[base + x], data).astype(BF16).reshape(2, 64, size)
            rows[base + x, :, :, pl.ds(first_col, size)] = chosen

    def products(chunk, tiles):
        start, first_col, size = DATA[chunk]
        for j in tiles:
            acc = sums_gu[j] if chunk else 0.0
            for h in range(2):
                left = rows[:, h, :, pl.ds(first_col, size)].reshape(512, size)
                acc = acc + dot(left, wgu[j, pl.ds(h * HALF + first_col, size), :])
            if chunk < len(DATA) - 1:
                sums_gu[j] = acc
                continue
            v, u = acc[:, :width], acc[:, width:]
            act = v / (1.0 + jnp.exp(-v)) * u * scale[...].reshape(512, width)
            hidden[:, pl.ds(j * width, width)] = act.astype(BF16)

    gathers[2].relay3()
    route(mine, 0)
    select(mine, 0, 0)
    route_back(mine, 0)
    gathers[0].wait_across()
    route(other, SIDE)
    select(other, SIDE, 0)
    for copy in loads:
        copy.wait()
    products(0, range(4))
    gathers[1].finish()
    products(0, range(4, ff_tiles))
    gathers[2].finish()
    select(mine, 0, 1)
    route_back(other, SIDE)
    gathers[1].wait_across()
    select(other, SIDE, 1)
    select(mine, 0, 2)
    products(1, range(ff_tiles))
    gathers[2].wait_across()
    select(other, SIDE, 2)
    products(2, range(ff_tiles))

    def project(k):
        for h in range(2):
            y = dot(hidden[...], wd[:, pl.ds(h * HALF + k * TILE, TILE)]).astype(BF16)
            rows[:, h, :, pl.ds(k * TILE, TILE)] = y.reshape(8, 64, TILE)

    def scatter(k, target, base):
        cols = pl.ds(k * TILE, TILE)
        for x in range(SIDE):
            y = rows[base + x, :, :, cols].reshape(128, TILE)
            placed = dot(place_t[base + x], y).astype(BF16)
            target[x, :, :, :, cols] = placed.reshape(SIDE, SIDE, 16, TILE)

    def sums(part, fixed):
        return (*pick(fixed), ALL, pl.ds(part * TILE, TILE))

    def add(part, fixed, pieces):
        index = sums(part, fixed)
        total = keep[index].astype(F32)
        for ref, where in pieces:
            total = total + ref[where].astype(F32)
        keep[index] = total.astype(BF16)

    def merge(part):
        for x in range(SIDE):
            add(part, {0: x}, [(got, sums(part, {0: x}))])

    sum_base = len(GATHER) * GATHER_SEMS

    def arrival(k, what):
        return sum_base + k * SUM_SEMS + what

    def line(ref, k, at2):
        f1, f2, f3 = ORDERS[k % 3]
        index = [ALL] * len(ref.shape)
        index[1 + [d for d in range(3) if d != f1].index(f2)] = at2
        return ref.at[tuple(index)]

    def into(ref, k, offset, way, h):
        f1, f2, f3 = ORDERS[k % 3]
        index = {f2: place.at(f2, offset)}
        if h is not None:
            index[f3] = pl.ds(2 * h, 2)
        return (way, *(index.get(d, ALL) for d in range(3) if d != f1))

    def half_line(k, step, offset, h):
        f1, f2, f3 = ORDERS[k % 3]
        return {f1: place.at(f1, step), f2: place.at(f2, offset), f3: pl.ds(2 * h, 2)}

    def open_first(k, offsets, base):
        f1 = ORDERS[k % 3][0]
        for h, step in FIRST:
            for offset in offsets:
                src = keep.at[sums(k, half_line(k, 2, offset, h))]
                dst = relay1[k].at[into(relay1[k], k, offset, h, None)]
                send(src, dst, place.device(f1, step), 5, base)
        for way, h, step in ((0, 1, 1), (1, 0, 3)):
            for offset in offsets:
                src = keep.at[sums(k, half_line(k, step, offset, h))]
                dst = final1[k].at[into(final1[k], k, offset, way, h)]
                send(src, dst, place.device(f1, step), 5, base + 1)

    def pass_on(k, offsets, base):
        for h, step in FIRST:
            for offset in offsets:
                where = half_line(k, step, offset, h)
                add(k, where, [(relay1[k], into(relay1[k], k, offset, h, None))])
                dst = final1[k].at[into(final1[k], k, offset, h, h)]
                send(
                    keep.at[sums(k, where)], dst, place.device(ORDERS[k % 3][0], step), 5, base + 1
                )

    def take_in(k, offsets):
        f1, f2, f3 = ORDERS[k % 3]
        for offset in offsets:
            where = {f1: place.own[f1], f2: place.at(f2, offset)}
            add(k, where, [(final1[k], into(final1[k], k, offset, way, None)) for way in range(2)])

    def open_second(k):
        dim, cut, fixed = second_ring(k)
        for h, step in FIRST:
            src = keep.at[sums(k, {**fixed, cut: pl.ds(2 * h, 2), dim: place.at(dim, 2)})]
            send(src, relay2[k].at[h], place.device(dim, step), 6, arrival(k, 3))
        for way, h, step in ((0, 1, 1), (1, 0, 3)):
            src = keep.at[sums(k, {**fixed, cut: pl.ds(2 * h, 2), dim: place.at(dim, step)})]
            dst = final2[k].at[way, pl.ds(2 * h, 2)]
            send(src, dst, place.device(dim, step), 6, arrival(k, 4))

    def second_ring(k):
        f1, f2, f3 = ORDERS[k % 3]
        return f2, f3, {f1: place.own[f1]}

    def compute(k):
        project(k)
        scatter(k, give, SIDE)
        piece = sums(k, {})
        send(give.at[piece], got.at[piece], partner, 4, arrival(k, 0))
        scatter(k, keep, 0)

    def begin(k):
        arrive(got.at[sums(k, {})], arrival(k, 0))
        merge(k)
        open_first(k, AROUND, arrival(k, 1))

    def pass_first(k):
        arrive(line(relay1[k], k, pl.ds(0, 3)), arrival(k, 1))
        pass_on(k, AROUND, arrival(k, 1))

    def close_first(k):
        arrive(line(final1[k], k, pl.ds(0, 3)), arrival(k, 2))
        take_in(k, AROUND)
        if k < DIRECT:
            open_second(k)
            return
        f1, f2, f3 = ORDERS[k % 3]
        for step in (1, 3, 2):
            src = keep.at[sums(k, {f1: place.own[f1], f2: place.at(f2, step)})]
            send(src, final2[k].at[step - 1], place.device(f2, step), 6, arrival(k, 4))

    def open_late(k):
        open_first(k, (0,), arrival(k, 6))

    def pass_late(k):
        arrive(line(relay1[k], k, 0), arrival(k, 6))
        pass_on(k, (0,), arrival(k, 6))

    def close_late(k):
        arrive(line(final1[k], k, 0), arrival(k, 7))
        take_in(k, (0,))

    def pass_second(k):
        if k >= DIRECT:
            return
        dim, cut, fixed = second_ring(k)
        arrive(relay2[k], arrival(k, 3))
        for h, step in FIRST:
            where = {**fixed, cut: pl.ds(2 * h, 2), dim: place.at(dim, step)}
            add(k, where, [(relay2[k], (h,))])
            dst = final2[k].at[h, pl.ds(2 * h, 2)]
            send(keep.at[sums(k, where)], dst, place.device(dim, step), 6, arrival(k, 4))

    def close_second(k):
        arrive(final2[k], arrival(k, 4))
        f1, f2, f3 = ORDERS[k % 3]
        ways = range(final2[k].shape[0])
        add(k, {f1: place.own[f1], f2: place.own[f2]}, [(final2[k], (i,)) for i in ways])
        f1, f2, f3 = ORDERS[k % 3]
        for step in (1, 3, 2):
            where = {f1: place.own[f1], f2: place.own[f2], f3: place.at(f3, step)}
            src = keep.at[sums(k, where)]
            send(src, last[k].at[step - 1], place.device(f3, step), 7, arrival(k, 5))

    def finish(k):
        arrive(last[k], arrival(k, 5))
        total = keep[sums(k, dict(enumerate(place.own)))].astype(F32)
        for i in range(3):
            total = total + last[k][i].astype(F32)
        out_ref[:, pl.ds(k * TILE, TILE)] = total[0:8].astype(BF16)
        out_ref[:, pl.ds(HALF + k * TILE, TILE)] = total[8:16].astype(BF16)
        for h in range(2):
            cols = pl.ds(h * HALF + k * TILE, TILE)
            pltpu.make_async_copy(out_ref.at[:, cols], out_hbm.at[:, cols], in_sems.at[3]).start()

    plan = []
    for k in range(CHUNKS):
        plan.append((1.1 * k, compute, k))
        plan.append((1.1 * k + 2.25, begin, k))
        closed = 11.8 + 0.85 * k
        second = max(closed + (6.2 if k < DIRECT else 4.2), 19.3 + 0.45 * k)
        plan.append((7.3 + 0.9 * k, pass_first, k))
        plan.append((closed, close_first, k))
        plan.append((closed + 3.1, pass_second, k))
        plan.append((11.0 + 0.5 * k, open_late, k))
        plan.append((15.5 + 0.5 * k, pass_late, k))
        plan.append((19.0 + 0.45 * k, close_late, k))
        plan.append((second, close_second, k))
        plan.append((second + 4.0, finish, k))
    for when, step, k in sorted(plan, key=lambda entry: entry[0]):
        step(k)

    pltpu.make_async_copy(out_ref, out_hbm, in_sems.at[3]).wait()

    for kind, sent in enumerate(
        (
            mine.at[pl.ds(0, 3), 0, 0], mine.at[pl.ds(0, 3), :, 0], mine.at[pl.ds(0, 3)], mine,
            keep, keep.at[pl.ds(0, 3)], keep.at[pl.ds(0, 3), :, 0], keep.at[pl.ds(0, 3), 0, 0],
        )
    ):
        waiting(sent, kind, 0).wait_send()


def ring_buffers():
    relay1, final1, relay2, final2, last = [], [], [], [], []
    for k in range(CHUNKS):
        f1, f2, f3 = ORDERS[k % 3]
        left = [d for d in range(3) if d != f1]
        relay1.append(pltpu.VMEM((2, *(2 if d == f3 else SIDE for d in left), 16, TILE), BF16))
        final1.append(pltpu.VMEM((2, SIDE, SIDE, 16, TILE), BF16))
        relay2.append(pltpu.VMEM((2, 2, 16, TILE), BF16))
        final2.append(pltpu.VMEM((2 if k < DIRECT else 3, SIDE, 16, TILE), BF16))
        last.append(pltpu.VMEM((3, 16, TILE), BF16))
    return relay1, final1, relay2, final2, last


def layer(tokens, router, expert_ids, w_gate, w_up, w_down):
    depth, ff = w_gate.shape[1], w_gate.shape[2]
    blocks = (SIDE, SIDE, SIDE, 16)
    anywhere = pl.BlockSpec(memory_space=pl.ANY)
    return pl.pallas_call(
        layer_kernel,
        out_shape=jax.ShapeDtypeStruct(tokens.shape, BF16),
        in_specs=[anywhere] * 6,
        out_specs=anywhere,
        scratch_shapes=[
            pltpu.VMEM(tokens.shape, BF16),
            pltpu.VMEM(router.shape[::-1], BF16),
            pltpu.VMEM(expert_ids.shape[::-1], jnp.int32),
            pltpu.VMEM(tokens.shape, BF16),
            pltpu.VMEM((ff // (TILE // 2), depth, TILE), BF16),
            pltpu.VMEM((ff, depth), BF16),
            pltpu.VMEM((*blocks, HALF + INFO), BF16),
            pltpu.VMEM((*blocks, HALF + INFO), BF16),
            pltpu.VMEM((8, 2, 64, HALF), BF16),
            pltpu.VMEM((8, 64, TILE // 2), F32),
            pltpu.VMEM((8, 128, 256), BF16),
            pltpu.VMEM((8, 256, 128), BF16),
            pltpu.VMEM((ff // (TILE // 2), 512, TILE), F32),
            pltpu.VMEM((512, ff), BF16),
            pltpu.VMEM((*blocks, HALF), BF16),
            pltpu.VMEM((*blocks, HALF), BF16),
            pltpu.VMEM((*blocks, HALF), BF16),
            *ring_buffers(),
            pltpu.SemaphoreType.DMA((4,)),
            pltpu.SemaphoreType.DMA((2 * (ff // (TILE // 2)) + 1,)),
            pltpu.SemaphoreType.DMA((8,)),
            pltpu.SemaphoreType.DMA((len(GATHER) * GATHER_SEMS + CHUNKS * SUM_SEMS,)),
        ],
        compiler_params=pltpu.CompilerParams(
            collective_id=0, has_side_effects=True, vmem_limit_bytes=67043328
        ),
    )(tokens, router.T, expert_ids.T, w_gate, w_up, w_down)


def solution(mesh):
    placed = (
        P(("expert", "shard"), None),
        P(),
        P(("expert", "shard"), None),
        P("expert", None, "shard"),
        P("expert", None, "shard"),
        P("expert", "shard", None),
    )
    return jax.shard_map(
        layer, mesh=mesh, in_specs=placed, out_specs=P(("expert", "shard"), None), check_vma=False
    )
```
